32 devices in a mesh: row: 4 (over y, x), col: 8 (over z, core).
Axes of the slice: x: 2, y: 2, z: 4, core: 2. Of those that a mesh axis runs over, the one named last changes fastest.
Arguments:
- train_table: bfloat16 [4, 256, 262144], P('row', 'col'), may hold values from -6 to 6
- token_ids: int32 [256], replicated, may hold values from 0 to 262143
- hidden: bfloat16 [4, 256, 2560], P('row', 'col'), may hold values from -6 to 6
- w_gate: bfloat16 [4, 2560, 256], P('row'), may hold values from -0.125 to 0.125
- w_proj: bfloat16 [4, 256, 2560], P('row'), may hold values from -0.375 to 0.375
- gain: bfloat16 [4, 2560], P('row'), may hold values from 0.5 to 1.5
Outputs:
- serve_table: bfloat16 [4, 256, 262144], P(None, None, ('row', 'col'))
- update: bfloat16 [4, 256, 2560], P('row', 'col')
The draws below stay inside these ranges and needn't reach their ends.
All inputs are finite; a program needn't handle non-finite values.
Results may differ from the reference program's by a relative error of at most 0.0048.
Values may be sent and summed in bfloat16 or wider, within the bound.
A program may use at most 256 MiB of HBM per device.

```python
import jax
import jax.numpy as jnp
from jax import lax

VOCAB = 262144
P_SIZE = 256
D = 2560
L = 4
TOKENS = 256


def touch_ends(array, stream_key, least, largest):
    longest = array.shape.index(max(array.shape))
    spots = []
    for shift in (0, 1):
        where = [jax.random.randint(jax.random.fold_in(stream_key, axis), (), 0, length) for axis, length in enumerate(array.shape)]
        where[longest] = (where[longest] + shift) % array.shape[longest]
        spots.append(tuple(where))
    return array.at[spots[0]].set(least).at[spots[1]].set(largest)


def levels(own_key, extent, shards, smallest, high):
    level = 1.0
    for axis_at, blocks in shards:
        heights = jax.random.uniform(jax.random.fold_in(jax.random.fold_in(own_key, 6), axis_at), (blocks,), jnp.float32, smallest / len(shards), high / len(shards))
        level = level * jnp.repeat(jnp.exp(heights), extent[axis_at] // blocks).reshape((-1,) + (1,) * (len(extent) - 1 - axis_at))
    return level


def gaussian(own_key, dims, scale, most, cuts=(), kind=jnp.bfloat16):
    entries = jax.random.normal(own_key, dims, jnp.float32) * scale
    if len(cuts) > 0:
        entries = levels(own_key, dims, cuts, -0.22, 0.18) * entries
    return jnp.clip(entries, min=-most, max=most).astype(kind)


def setup_inputs(seed: int = 0) -> dict:
    arg_keys = jax.random.split(jax.random.key(seed), 7)
    return {
        "train_table": gaussian(arg_keys[0], (L, P_SIZE, VOCAB), 1.0, 6.0, ((0, 4), (1, 8))),
        "token_ids": touch_ends(jax.random.randint(arg_keys[1], (TOKENS,), 0, VOCAB), jax.random.fold_in(arg_keys[1], 1), 0, VOCAB - 1).astype(jnp.int32),
        "hidden": gaussian(arg_keys[2], (L, TOKENS, D), 1.0, 6.0, ((0, 4), (1, 8))),
        "w_gate": gaussian(arg_keys[3], (L, D, P_SIZE), D ** -0.5, 0.125, ((0, 4),)),
        "w_proj": gaussian(arg_keys[4], (L, P_SIZE, D), P_SIZE ** -0.5, 0.375, ((0, 4),)),
        "gain": jnp.clip(1.0 + 0.1 * jax.random.normal(arg_keys[5], (L, D), jnp.float32), 0.5, 1.5).astype(jnp.bfloat16),
    }


def reference(train_table, token_ids, hidden, w_gate, w_proj, gain):
    emb = jnp.take(train_table, token_ids.astype(jnp.int32), axis=2).astype(jnp.float32)
    emb = jnp.transpose(emb, (0, 2, 1))
    gate_pre = jnp.einsum('ltd,ldp->ltp', hidden.astype(jnp.float32), w_gate.astype(jnp.float32))
    gated = jax.nn.gelu(gate_pre, approximate=True)
    mixed = (gated * emb).astype(jnp.bfloat16)
    projected = jnp.einsum('ltp,lpd->ltd', mixed.astype(jnp.float32), w_proj.astype(jnp.float32))
    inverse_rms = jax.lax.rsqrt(lax.optimization_barrier(jnp.mean(projected * projected, axis=-1, keepdims=True)) + 1e-06)
    update = (projected * inverse_rms * gain.astype(jnp.float32)[:, None, :]).astype(jnp.bfloat16)
    return (train_table, update)
```

```python
import functools

import jax
import jax.numpy as jnp
from jax import lax
from jax.experimental import pallas as pl
from jax.experimental.pallas import tpu as pltpu
from jax.sharding import PartitionSpec as P

MESH = pl.DeviceIdType.MESH


def gather_kernel(ids_ref, table_ref, tiles_ref, sem):
    def fetch(i, carry):
        start = pl.multiple_of(lax.div(ids_ref[i], 128) * 128, 128)
        pltpu.make_async_copy(table_ref.at[0, :, pl.ds(start, 128)], tiles_ref.at[i], sem).start()
        return carry
    lax.fori_loop(0, tiles_ref.shape[0], fetch, 0, unroll=8)
    pltpu.make_async_copy(tiles_ref, tiles_ref, sem).wait()


def exchange_kernel(
    rows, cols, ids_ref, tiles_ref, table_ref, hidden_ref, w_gate_ref, w_proj_ref, gain_ref,
    served_ref, update_ref,
    own, hidden, w_gate, w_proj, gain, picked, arrived,
    send_sem, recv_sem, emb_send_sem, emb_recv_sem, local_sem,
):
    total = rows * cols
    columns = table_ref.shape[1]
    local_vocab = table_ref.shape[2] // total
    tokens = hidden_ref.shape[1]
    lanes = picked.shape[2]
    my_row, my_col = lax.axis_index("row"), lax.axis_index("col")
    me = my_row * cols + my_col
    side = 1 - 2 * (my_col // (cols // 2))

    def place(row, col):
        start = pl.multiple_of(col * columns, columns)
        return served_ref.at[row, pl.ds(start, columns), :]

    def block(rank):
        return pl.ds(pl.multiple_of(rank * local_vocab, local_vocab), local_vocab)

    loads = [
        pltpu.make_async_copy(src, dst, local_sem.at[i])
        for i, (src, dst) in enumerate((
            (hidden_ref.at[0], hidden),
            (w_gate_ref.at[0], w_gate),
            (w_proj_ref.at[0], w_proj),
            (gain_ref, gain),
            (table_ref.at[0, :, block(me)], own),
        ))
    ]
    for load in loads:
        load.start()

    def peer(k):
        row = (my_row + k % rows) % rows
        col = (my_col + side * (k // rows) + cols) % cols
        return row, col

    def send(k):
        row, col = peer(k)
        return pltpu.make_async_remote_copy(
            src_ref=table_ref.at[0, :, block(row * cols + col)],
            dst_ref=place(my_row, my_col),
            send_sem=send_sem.at[k],
            recv_sem=recv_sem.at[me],
            device_id=(row, col),
            device_id_type=MESH,
        )

    def receive(k):
        row, col = peer(k)
        return pltpu.make_async_remote_copy(
            src_ref=table_ref.at[0, :, block(row * cols + col)],
            dst_ref=place(row, col),
            send_sem=send_sem.at[k],
            recv_sem=recv_sem.at[row * cols + col],
            device_id=(row, col),
            device_id_type=MESH,
        )

    def send_emb(k):
        col = (my_col + k) % cols
        return pltpu.make_async_remote_copy(
            src_ref=picked.at[col],
            dst_ref=arrived.at[my_col],
            send_sem=emb_send_sem.at[k],
            recv_sem=emb_recv_sem.at[k],
            device_id=(my_row, col),
            device_id_type=MESH,
        )

    def receive_emb(k):
        col = (my_col + cols - k) % cols
        return pltpu.make_async_remote_copy(
            src_ref=picked.at[col],
            dst_ref=arrived.at[col],
            send_sem=emb_send_sem.at[k],
            recv_sem=emb_recv_sem.at[k],
            device_id=(my_row, col),
            device_id_type=MESH,
        )

    def each(first, last, act):
        def body(k, carry):
            act(k)
            return carry
        lax.fori_loop(first, last, body, 0)

    barrier = pltpu.get_barrier_semaphore()

    def greet(k):
        pl.semaphore_signal(barrier, inc=1, device_id=peer(k), device_id_type=MESH)

    each(1, total, greet)
    pl.semaphore_wait(barrier, total - 1)

    half = total // 2
    each(1, half, lambda k: send(k).start())

    lane = lax.broadcasted_iota(jnp.int32, (columns, 128), 1)
    spot = lax.broadcasted_iota(jnp.int32, (columns, lanes), 1)

    def pick(col):
        def body(j, gathered):
            at = col * tokens + j
            tile = tiles_ref[at].astype(jnp.float32)
            wanted = lane == lax.rem(ids_ref[at], 128)
            value = jnp.sum(jnp.where(wanted, tile, 0.0), axis=1, keepdims=True)
            return jnp.where(spot == j, value, gathered)
        gathered = lax.fori_loop(0, tokens, body, jnp.zeros((columns, lanes), jnp.float32))
        picked[col] = gathered.astype(jnp.bfloat16)

    each(0, cols, pick)

    for load in loads:
        load.wait()
    keep = pltpu.make_async_copy(own, place(my_row, my_col), local_sem.at[len(loads)])
    keep.start()
    gate_pre = jnp.dot(hidden[...], w_gate[...], preferred_element_type=jnp.float32)
    gated = jax.nn.gelu(gate_pre, approximate=True)

    each(1, cols, lambda k: send_emb(k).start())
    each(half, total, lambda k: send(k).start())

    arrived[my_col] = picked[my_col]
    each(1, cols, lambda k: receive_emb(k).wait_recv())
    flat = arrived[...].astype(jnp.float32).reshape(cols * columns, lanes)
    emb = jnp.transpose(flat)[:tokens, :]
    mixed = (gated * emb).astype(jnp.bfloat16)
    projected = jnp.dot(mixed, w_proj[...], preferred_element_type=jnp.float32)
    inverse_rms = lax.rsqrt(jnp.mean(projected * projected, axis=-1, keepdims=True) + 1e-06)
    scaled = projected * inverse_rms * gain[...].astype(jnp.float32)
    update_ref[0] = scaled.astype(jnp.bfloat16)

    each(1, cols, lambda k: send_emb(k).wait_send())
    keep.wait()
    each(1, total, lambda k: receive(k).wait_recv())
    each(1, total, lambda k: send(k).wait_send())


def shards(train_table, token_ids, hidden, w_gate, w_proj, gain):
    rows = lax.axis_size("row")
    cols = lax.axis_size("col")
    total = rows * cols
    columns, vocab = train_table.shape[1:]
    tokens, width = hidden.shape[1:]
    p_size = w_gate.shape[2]
    lanes = -(-tokens // 128) * 128
    anywhere = pl.BlockSpec(memory_space=pl.ANY)
    tiles = pl.pallas_call(
        gather_kernel,
        out_shape=jax.ShapeDtypeStruct((token_ids.shape[0], columns, 128), train_table.dtype),
        in_specs=[pl.BlockSpec(memory_space=pltpu.SMEM), anywhere],
        out_specs=pl.BlockSpec(memory_space=pltpu.VMEM),
        scratch_shapes=[pltpu.SemaphoreType.DMA],
    )(token_ids, train_table)
    served, update = pl.pallas_call(
        functools.partial(exchange_kernel, rows, cols),
        out_shape=(
            jax.ShapeDtypeStruct((rows, cols * columns, vocab // total), train_table.dtype),
            jax.ShapeDtypeStruct(hidden.shape, jnp.bfloat16),
        ),
        in_specs=[pl.BlockSpec(memory_space=pltpu.SMEM), pl.BlockSpec(memory_space=pltpu.VMEM)] + [anywhere] * 5,
        out_specs=(anywhere, pl.BlockSpec(memory_space=pltpu.VMEM)),
        scratch_shapes=[
            pltpu.VMEM((columns, vocab // total), jnp.bfloat16),
            pltpu.VMEM((tokens, width), jnp.bfloat16),
            pltpu.VMEM((width, p_size), jnp.bfloat16),
            pltpu.VMEM((p_size, width), jnp.bfloat16),
            pltpu.VMEM((1, width), jnp.bfloat16),
            pltpu.VMEM((cols, columns, lanes), jnp.bfloat16),
            pltpu.VMEM((cols, columns, lanes), jnp.bfloat16),
            pltpu.SemaphoreType.DMA((total,)),
            pltpu.SemaphoreType.DMA((total,)),
            pltpu.SemaphoreType.DMA((cols,)),
            pltpu.SemaphoreType.DMA((cols,)),
            pltpu.SemaphoreType.DMA((6,)),
        ],
        compiler_params=pltpu.CompilerParams(collective_id=0, has_side_effects=True),
    )(token_ids, tiles, train_table, hidden, w_gate, w_proj, gain)
    return (served, update)


def solution(mesh):
    in_specs = (
        P("row", "col", None),
        P(),
        P("row", "col", None),
        P("row", None, None),
        P("row", None, None),
        P("row", None),
    )
    out_specs = (P(None, None, ("row", "col")), P("row", "col", None))
    return jax.shard_map(shards, mesh=mesh, in_specs=in_specs, out_specs=out_specs, check_vma=False)
```

```python
import functools

import jax
import jax.numpy as jnp
from jax import lax
from jax.experimental import pallas as pl
from jax.experimental.pallas import tpu as pltpu
from jax.sharding import PartitionSpec as P

MESH = pl.DeviceIdType.MESH


def gather_kernel(ids_ref, table_ref, tiles_ref, sem):
    def fetch(i, carry):
        start = pl.multiple_of(lax.div(ids_ref[i], 128) * 128, 128)
        pltpu.make_async_copy(table_ref.at[0, :, pl.ds(start, 128)], tiles_ref.at[i], sem).start()
        return carry
    lax.fori_loop(0, tiles_ref.shape[0], fetch, 0, unroll=8)
    pltpu.make_async_copy(tiles_ref, tiles_ref, sem).wait()


def exchange_kernel(
    rows, cols, ids_ref, tiles_ref, table_ref, hidden_ref, w_gate_ref, w_proj_ref, gain_ref,
    served_ref, update_ref, late_ref,
    own, late, hidden, w_gate, w_proj, gain, picked, arrived,
    send_sem, recv_sem, emb_send_sem, emb_recv_sem, local_sem,
):
    total = rows * cols
    columns = table_ref.shape[1]
    local_vocab = table_ref.shape[2] // total
    tokens = hidden_ref.shape[1]
    lanes = picked.shape[2]
    my_row, my_col = lax.axis_index("row"), lax.axis_index("col")
    me = my_row * cols + my_col
    side = 1 - 2 * (my_col // (cols // 2))
    core = my_col % 2

    def place(row, col):
        start = pl.multiple_of(col * columns, columns)
        return served_ref.at[row, pl.ds(start, columns), :]

    def block(rank):
        return pl.ds(pl.multiple_of(rank * local_vocab, local_vocab), local_vocab)

    loads = [
        pltpu.make_async_copy(src, dst, local_sem.at[i])
        for i, (src, dst) in enumerate((
            (hidden_ref.at[0], hidden),
            (w_gate_ref.at[0], w_gate),
            (w_proj_ref.at[0], w_proj),
            (gain_ref, gain),
            (table_ref.at[0, :, block(me)], own),
            (table_ref.at[0, :, block(my_row * cols + (my_col + cols // 2) % cols)], late),
        ))
    ]
    for load in loads:
        load.start()

    def peer(k):
        k = core * (total - k) + (1 - core) * k
        row = (my_row + k % rows) % rows
        col = (my_col + side * (k // rows) + cols) % cols
        return row, col

    def send(k):
        row, col = peer(k)
        return pltpu.make_async_remote_copy(
            src_ref=table_ref.at[0, :, block(row * cols + col)],
            dst_ref=place(my_row, my_col),
            send_sem=send_sem.at[k],
            recv_sem=recv_sem.at[me],
            device_id=(row, col),
            device_id_type=MESH,
        )

    def receive(k):
        row, col = peer(k)
        return pltpu.make_async_remote_copy(
            src_ref=table_ref.at[0, :, block(row * cols + col)],
            dst_ref=place(row, col),
            send_sem=send_sem.at[k],
            recv_sem=recv_sem.at[row * cols + col],
            device_id=(row, col),
            device_id_type=MESH,
        )

    def send_emb(k):
        col = (my_col + k) % cols
        return pltpu.make_async_remote_copy(
            src_ref=picked.at[col],
            dst_ref=arrived.at[my_col],
            send_sem=emb_send_sem.at[k],
            recv_sem=emb_recv_sem.at[k],
            device_id=(my_row, col),
            device_id_type=MESH,
        )

    def receive_emb(k):
        col = (my_col + cols - k) % cols
        return pltpu.make_async_remote_copy(
            src_ref=picked.at[col],
            dst_ref=arrived.at[col],
            send_sem=emb_send_sem.at[k],
            recv_sem=emb_recv_sem.at[k],
            device_id=(my_row, col),
            device_id_type=MESH,
        )

    def each(first, last, act):
        def body(k, carry):
            act(k)
            return carry
        lax.fori_loop(first, last, body, 0)

    barrier = pltpu.get_barrier_semaphore()

    def greet(k):
        pl.semaphore_signal(barrier, inc=1, device_id=peer(k), device_id_type=MESH)

    each(1, total, greet)
    pl.semaphore_wait(barrier, total - 1)

    half = total // 2
    cut = total * 3 // 4
    each(1, half, lambda k: send(k).start())
    each(half + 1, cut, lambda k: send(k).start())

    lane = lax.broadcasted_iota(jnp.int32, (columns, 128), 1)
    spot = lax.broadcasted_iota(jnp.int32, (columns, lanes), 1)

    def pick(col):
        def body(j, gathered):
            at = col * tokens + j
            tile = tiles_ref[at].astype(jnp.float32)
            wanted = lane == lax.rem(ids_ref[at], 128)
            value = jnp.sum(jnp.where(wanted, tile, 0.0), axis=1, keepdims=True)
            return jnp.where(spot == j, value, gathered)
        gathered = lax.fori_loop(0, tokens, body, jnp.zeros((columns, lanes), jnp.float32))
        picked[col] = gathered.astype(jnp.bfloat16)

    each(0, cols, pick)

    for load in loads:
        load.wait()
    keep = pltpu.make_async_copy(own, place(my_row, my_col), local_sem.at[len(loads)])
    keep.start()
    put = pltpu.make_async_copy(late, late_ref, local_sem.at[len(loads) + 1])
    put.start()
    gate_pre = jnp.dot(hidden[...], w_gate[...], preferred_element_type=jnp.float32)
    gated = jax.nn.gelu(gate_pre, approximate=True)

    each(1, cols, lambda k: send_emb(k).start())
    each(cut, total, lambda k: send(k).start())

    arrived[my_col] = picked[my_col]
    each(1, cols, lambda k: receive_emb(k).wait_recv())
    flat = arrived[...].astype(jnp.float32).reshape(cols * columns, lanes)
    emb = jnp.transpose(flat)[:tokens, :]
    mixed = (gated * emb).astype(jnp.bfloat16)
    projected = jnp.dot(mixed, w_proj[...], preferred_element_type=jnp.float32)
    inverse_rms = lax.rsqrt(jnp.mean(projected * projected, axis=-1, keepdims=True) + 1e-06)
    scaled = projected * inverse_rms * gain[...].astype(jnp.float32)
    update_ref[0] = scaled.astype(jnp.bfloat16)

    each(1, cols, lambda k: send_emb(k).wait_send())
    keep.wait()
    put.wait()
    for first, last in ((1, half), (half + 1, total)):
        each(first, last, lambda k: receive(k).wait_recv())
        each(first, last, lambda k: send(k).wait_send())


def copy_kernel(served_ref, update_ref, served_out_ref, update_out_ref):
    served_out_ref[...] = served_ref[...]
    update_out_ref[...] = update_ref[...]


def settle(served, update):
    rows, depth, width = served.shape
    step = depth // 4
    table = pl.BlockSpec((1, step, width), lambda i, j: (i, j, 0))
    small = pl.BlockSpec(update.shape, lambda i, j: (0, 0, 0))
    moved = 2 * (served.size + update.size) * served.dtype.itemsize
    return pl.pallas_call(
        copy_kernel,
        out_shape=tuple(jax.ShapeDtypeStruct(x.shape, x.dtype) for x in (served, update)),
        grid=(rows, depth // step),
        in_specs=[table, small],
        out_specs=(table, small),
        cost_estimate=pl.CostEstimate(flops=0, bytes_accessed=moved, transcendentals=0),
    )(served, update)


def shards(train_table, token_ids, hidden, w_gate, w_proj, gain):
    rows = lax.axis_size("row")
    cols = lax.axis_size("col")
    total = rows * cols
    columns, vocab = train_table.shape[1:]
    tokens, width = hidden.shape[1:]
    p_size = w_gate.shape[2]
    lanes = -(-tokens // 128) * 128
    anywhere = pl.BlockSpec(memory_space=pl.ANY)
    tiles = pl.pallas_call(
        gather_kernel,
        out_shape=jax.ShapeDtypeStruct((token_ids.shape[0], columns, 128), train_table.dtype),
        in_specs=[pl.BlockSpec(memory_space=pltpu.SMEM), anywhere],
        out_specs=pl.BlockSpec(memory_space=pltpu.VMEM),
        scratch_shapes=[pltpu.SemaphoreType.DMA],
    )(token_ids, train_table)
    served, update, late = pl.pallas_call(
        functools.partial(exchange_kernel, rows, cols),
        out_shape=(
            jax.ShapeDtypeStruct((rows, cols * columns, vocab // total), train_table.dtype),
            jax.ShapeDtypeStruct(hidden.shape, jnp.bfloat16),
            jax.ShapeDtypeStruct((columns, vocab // total), train_table.dtype),
        ),
        in_specs=[pl.BlockSpec(memory_space=pltpu.SMEM), pl.BlockSpec(memory_space=pltpu.VMEM)] + [anywhere] * 5,
        out_specs=(anywhere, pl.BlockSpec(memory_space=pltpu.VMEM), anywhere),
        scratch_shapes=[
            pltpu.VMEM((columns, vocab // total), jnp.bfloat16),
            pltpu.VMEM((columns, vocab // total), jnp.bfloat16),
            pltpu.VMEM((tokens, width), jnp.bfloat16),
            pltpu.VMEM((width, p_size), jnp.bfloat16),
            pltpu.VMEM((p_size, width), jnp.bfloat16),
            pltpu.VMEM((1, width), jnp.bfloat16),
            pltpu.VMEM((cols, columns, lanes), jnp.bfloat16),
            pltpu.VMEM((cols, columns, lanes), jnp.bfloat16),
            pltpu.SemaphoreType.DMA((total,)),
            pltpu.SemaphoreType.DMA((total,)),
            pltpu.SemaphoreType.DMA((cols,)),
            pltpu.SemaphoreType.DMA((cols,)),
            pltpu.SemaphoreType.DMA((8,)),
        ],
        compiler_params=pltpu.CompilerParams(collective_id=0, has_side_effects=True),
    )(token_ids, tiles, train_table, hidden, w_gate, w_proj, gain)
    shift = cols // 2
    came = lax.ppermute(late, "col", [(i, (i + shift) % cols) for i in range(cols)])
    served, update = settle(served, update)
    source = (lax.axis_index("col") + shift) % cols
    spot = (lax.axis_index("row"), source * columns, 0)
    served = lax.dynamic_update_slice(served, came[None], spot)
    return (served, update)


def solution(mesh):
    in_specs = (
        P("row", "col", None),
        P(),
        P("row", "col", None),
        P("row", None, None),
        P("row", None, None),
        P("row", None),
    )
    out_specs = (P(None, None, ("row", "col")), P("row", "col", None))
    return jax.shard_map(shards, mesh=mesh, in_specs=in_specs, out_specs=out_specs, check_vma=False)
```
